32 devices in a mesh: frag: 1 (over z), dev: 32 (over y, x, core).
Axes of the slice: x: 4, y: 4, z: 1, core: 2. Of those that a mesh axis runs over, the one named last changes fastest.
The devices are a block of a 4x4x8 slice.
Arguments:
- ao_ints: bfloat16 [160, 160, 160, 160], P(('frag', 'dev'))
- occ_coef: bfloat16 [160, 54], P('frag')
- virt_coef: bfloat16 [160, 64], P('frag')
Outputs:
- output: float32 [54, 64, 3456], P('frag', None, 'dev')
All inputs are finite; a program needn't handle non-finite values.
Results may differ from the reference program's by a relative error of at most 0.001.
Values are sent between devices in bfloat16 or wider.
A program may use at most 768 MiB of HBM per device.

```python
import jax
import jax.numpy as jnp
from jax import lax

AO_DIM = 160
OCC_DIM = 54
VIRT_DIM = 64


def setup_inputs(seed: int = 0, part: int = 0) -> dict:
    base_key = jax.random.fold_in(jax.random.key(seed), part)
    key_ints, key_occ, key_virt = jax.random.split(base_key, 3)
    row_keys = jax.random.split(key_ints, AO_DIM)

    def draw_row(row_key):
        return jax.random.normal(row_key, (AO_DIM, AO_DIM, AO_DIM), jnp.float32).astype(jnp.bfloat16)

    ao_ints = lax.map(draw_row, row_keys)
    coef_scale = AO_DIM ** -0.5
    occ_coef = jax.random.normal(key_occ, (AO_DIM, OCC_DIM), jnp.float32) * coef_scale
    virt_coef = jax.random.normal(key_virt, (AO_DIM, VIRT_DIM), jnp.float32) * coef_scale
    return {"ao_ints": ao_ints, "occ_coef": occ_coef.astype(jnp.bfloat16), "virt_coef": virt_coef.astype(jnp.bfloat16)}


def reference(ao_ints, occ_coef, virt_coef):
    occ_wide = occ_coef.astype(jnp.float32)
    virt_wide = virt_coef.astype(jnp.float32)

    def first_half(ao_row):
        quarter = jnp.einsum("qrs,rj->qsj", ao_row.astype(jnp.float32), occ_wide).astype(jnp.bfloat16)
        half_row = jnp.einsum("qsj,sb->qjb", quarter.astype(jnp.float32), virt_wide).astype(jnp.bfloat16)
        return half_row.reshape(AO_DIM, OCC_DIM * VIRT_DIM)

    half_ints = lax.map(first_half, ao_ints)
    three_quarter = jnp.einsum("qa,pqc->apc", virt_wide, half_ints.astype(jnp.float32)).astype(jnp.bfloat16)
    return jnp.einsum("pi,apc->iac", occ_wide, three_quarter.astype(jnp.float32))
```

```python
import functools

import jax
import jax.numpy as jnp
from jax import lax
from jax.experimental import pallas as pl
from jax.experimental.pallas import tpu as pltpu
from jax.sharding import PartitionSpec as P

MESH = pl.DeviceIdType.MESH
F32 = jnp.float32
BF16 = jnp.bfloat16
LANES = 128
CHUNK = 16
GROUP = 4
SLOTS = 8
SUB = 16


def dot(a, b):
    return jnp.dot(a, b, preferred_element_type=F32)


def dot_t(a, b):
    return lax.dot_general(a, b, (((1,), (1,)), ((), ())), preferred_element_type=F32)


def iota(shape, dim):
    return lax.broadcasted_iota(jnp.int32, shape, dim)


def one_hot(condition):
    return jnp.where(condition, 1.0, 0.0).astype(BF16)


def kernel(n, ao, co_t, cv_t, out, a_buf, h_buf, g_buf, s_buf, r_buf, kron, co_eo, cv_dup, a_sem, s_sem, r_sem):
    rows, ao_dim = ao.shape[0], ao.shape[1]
    occ, virt = co_t.shape[0], cv_t.shape[0]
    block = out.shape[2]
    half = 32
    pairs = occ // 2
    stride = h_buf.shape[0] // half
    chunks = ao_dim // CHUNK
    me = lax.axis_index("dev")
    barrier = pltpu.get_barrier_semaphore()

    def load(index):
        slot = lax.rem(index, SLOTS)
        return pltpu.make_async_copy(
            ao.at[index // chunks, pl.ds(lax.rem(index, chunks) * CHUNK, CHUNK)], a_buf.at[slot], a_sem.at[slot]
        )

    for index in range(SLOTS):
        load(jnp.int32(index)).start()

    @pl.loop(1, n)
    def _(k):
        pl.semaphore_signal(barrier, inc=1, device_id={"dev": lax.rem(me + k, n)}, device_id_type=MESH)

    row, col = iota((2 * half, occ), 0), iota((2 * half, occ), 1)
    want = jnp.where(row < half, 2 * row, 2 * (row - half) + 1)
    co_eo[...] = dot(one_hot(want == col), co_t[...]).astype(BF16)
    row, col = iota((2 * virt, virt), 0), iota((2 * virt, virt), 1)
    dup_t = dot(one_hot(lax.rem(row, virt) == col), cv_t[...]).astype(BF16)
    row, col = iota((ao_dim, ao_dim), 0), iota((ao_dim, ao_dim), 1)
    cv_dup[...] = dot_t(one_hot(row == col), dup_t).astype(BF16)

    lane = iota((half, LANES), 1)
    lane_v = iota((virt, LANES), 1)

    def row_step(p, carry):
        def chunk_step(ch, carry):
            index = p * chunks + ch
            slot = lax.rem(index, SLOTS)
            load(index).wait()
            for group in range(CHUNK // GROUP):
                quarter = [
                    dot(co_eo[...], a_buf[slot, group * GROUP + u]).astype(BF16) for u in range(GROUP)
                ]
                h = dot(jnp.concatenate(quarter, axis=0), cv_dup[...])
                for u in range(GROUP):
                    even = h[u * 2 * half : u * 2 * half + half]
                    odd = h[u * 2 * half + half : (u + 1) * 2 * half]
                    h_buf[pl.ds(ch * CHUNK + group * GROUP + u, half, stride=stride), :] = jnp.where(
                        lane < virt, even, odd
                    )

            @pl.when(index + SLOTS < rows * chunks)
            def _():
                load(index + SLOTS).start()

            return carry

        lax.fori_loop(0, chunks, chunk_step, 0)

        for first in range(0, pairs, 2):
            width = min(2, pairs - first)
            half_ints = jnp.concatenate(
                [h_buf[(first + w) * stride : (first + w) * stride + ao_dim, :].astype(BF16) for w in range(width)],
                axis=1,
            )
            g_buf[:, first * LANES : (first + width) * LANES] = dot(cv_t[...], half_ints)
        for d in range(n):
            start, offset = divmod(block * d, LANES)
            piece = g_buf[:, start * LANES : (start + 1) * LANES]
            if offset:
                piece = pltpu.roll(piece, LANES - offset, 1)
                if offset + block > LANES:
                    more = pltpu.roll(g_buf[:, (start + 1) * LANES : (start + 2) * LANES], LANES - offset, 1)
                    piece = jnp.where(lane_v < LANES - offset, piece, more)
            s_buf[p, d] = piece.astype(BF16)

        @pl.when(p == 0)
        def _():
            pl.semaphore_wait(barrier, n - 1)

        r_buf[p, me] = s_buf[p, me]

        @pl.loop(1, n)
        def _(k):
            to = lax.rem(me + k, n)
            pltpu.make_async_remote_copy(
                src_ref=s_buf.at[p, to],
                dst_ref=r_buf.at[p, me],
                send_sem=s_sem.at[p],
                recv_sem=r_sem.at[p],
                device_id={"dev": to},
                device_id_type=MESH,
            ).start()

        return carry

    lax.fori_loop(0, rows, row_step, 0)

    m, k = occ * SUB, n * SUB
    row, col = iota((m, occ), 0), iota((m, occ), 1)
    wide = dot(one_hot(row // SUB == col), co_t[...]).astype(BF16)
    same = lax.rem(iota((m, k), 0), SUB) == lax.rem(iota((m, k), 1), SUB)
    for p in range(rows):
        row, col = iota((ao_dim, k), 0), iota((ao_dim, k), 1)
        spread = dot(wide, one_hot((col // SUB) * rows + p == row))
        kron[p] = jnp.where(same, spread, 0.0).astype(BF16)

    def last(p, add):
        arrived = r_buf.at[p, pl.ds(0, n - 1)]
        pltpu.make_async_copy(arrived, arrived, r_sem.at[p]).wait()
        for first in range(0, virt // SUB, 2):
            three_quarter = jnp.concatenate(
                [
                    r_buf[p, :, (first + w) * SUB : (first + w + 1) * SUB, :].reshape(n * SUB, LANES)
                    for w in range(2)
                ],
                axis=1,
            )
            v = dot(kron[p], three_quarter)
            for w in range(2):
                a = (first + w) * SUB
                part = v[:, w * LANES : (w + 1) * LANES].reshape(occ, SUB, LANES)[:, :, :block]
                if add:
                    part = part + out[:, a : a + SUB, :]
                out[:, a : a + SUB, :] = part

    last(0, False)
    for p in range(1, rows):
        last(p, True)
    for p in range(rows):
        sent = s_buf.at[p, pl.ds(0, n - 1)]
        pltpu.make_async_copy(sent, sent, s_sem.at[p]).wait()


def solution(mesh):
    n = mesh.shape["dev"]

    def local_part(ao_rows, occ_coef, virt_coef):
        rows, ao_dim = ao_rows.shape[0], ao_rows.shape[1]
        occ, virt = occ_coef.shape[1], virt_coef.shape[1]
        block = occ * virt // n
        stride = ao_dim + 8
        vmem = pl.BlockSpec(memory_space=pltpu.VMEM)
        return pl.pallas_call(
            functools.partial(kernel, n),
            out_shape=jax.ShapeDtypeStruct((occ, virt, block), F32),
            in_specs=[pl.BlockSpec(memory_space=pl.ANY), vmem, vmem],
            out_specs=vmem,
            scratch_shapes=[
                pltpu.VMEM((SLOTS, CHUNK, ao_dim, ao_dim), BF16),
                pltpu.VMEM((32 * stride, LANES), F32),
                pltpu.VMEM((virt, (occ * virt // LANES) * LANES), F32),
                pltpu.VMEM((rows, n, virt, LANES), BF16),
                pltpu.VMEM((rows, n, virt, LANES), BF16),
                pltpu.VMEM((rows, occ * SUB, n * SUB), BF16),
                pltpu.VMEM((64, ao_dim), BF16),
                pltpu.VMEM((ao_dim, 2 * virt), BF16),
                pltpu.SemaphoreType.DMA((SLOTS,)),
                pltpu.SemaphoreType.DMA((rows,)),
                pltpu.SemaphoreType.DMA((rows,)),
            ],
            compiler_params=pltpu.CompilerParams(
                collective_id=0, has_side_effects=True, vmem_limit_bytes=56 * 1024 * 1024
            ),
            name="transform",
        )(ao_rows, occ_coef.T, virt_coef.T)

    return jax.shard_map(
        local_part,
        mesh=mesh,
        in_specs=(P(("frag", "dev"), None, None, None), P("frag", None), P("frag", None)),
        out_specs=P("frag", None, "dev"),
        check_vma=False,
    )
```

```python
import functools

import jax
import jax.numpy as jnp
from jax import lax
from jax.experimental import pallas as pl
from jax.experimental.pallas import tpu as pltpu
from jax.sharding import PartitionSpec as P

MESH = pl.DeviceIdType.MESH
F32 = jnp.float32
BF16 = jnp.bfloat16
LANES = 128
SUB = 8
CHUNK = 16
GROUP = 4
SLOTS = 8
HALF = 32


def dot(a, b):
    return jnp.dot(a, b, preferred_element_type=F32)


def dot_t(a, b):
    return lax.dot_general(a, b, (((1,), (1,)), ((), ())), preferred_element_type=F32)


def iota(shape, dim):
    return lax.broadcasted_iota(jnp.int32, shape, dim)


def one_hot(condition):
    return jnp.where(condition, 1.0, 0.0).astype(BF16)


def fold_plan(block):
    count = -(-block // (LANES - block))
    assert block % count == 0
    return count, block // count


def kernel(
    n, ao, co_in, cv_in, out, co_t, cv_t, a_buf, t_buf, h_buf, g_buf, s_buf, r_buf, acc, kron, co_eo, cv_dup,
    c_sem, a_sem, s_sem, r_sem,
):
    rows, ao_dim = ao.shape[0], ao.shape[1]
    occ, virt = co_in.shape[0], cv_in.shape[0]
    block = out.shape[2]
    count, width = fold_plan(block)
    kept = virt - SUB
    pairs = occ // 2
    stride = h_buf.shape[0] // HALF
    chunks = ao_dim // CHUNK
    me = lax.axis_index("dev")
    barrier = pltpu.get_barrier_semaphore()

    coef = [pltpu.make_async_copy(co_in, co_t, c_sem.at[0]), pltpu.make_async_copy(cv_in, cv_t, c_sem.at[1])]
    for copy in coef:
        copy.start()

    def load(index):
        slot = lax.rem(index, SLOTS)
        return pltpu.make_async_copy(
            ao.at[index // chunks, pl.ds(lax.rem(index, chunks) * CHUNK, CHUNK)], a_buf.at[slot], a_sem.at[slot]
        )

    for index in range(SLOTS):
        load(jnp.int32(index)).start()

    @pl.loop(1, n)
    def _(k):
        pl.semaphore_signal(barrier, inc=1, device_id={"dev": lax.rem(me + k, n)}, device_id_type=MESH)

    for copy in coef:
        copy.wait()
    row, col = iota((2 * HALF, occ), 0), iota((2 * HALF, occ), 1)
    want = jnp.where(row < HALF, 2 * row, 2 * (row - HALF) + 1)
    co_eo[...] = dot(one_hot(want == col), co_t[...]).astype(BF16)
    row, col = iota((2 * virt, virt), 0), iota((2 * virt, virt), 1)
    dup_t = dot(one_hot(lax.rem(row, virt) == col), cv_t[...]).astype(BF16)
    row, col = iota((ao_dim, ao_dim), 0), iota((ao_dim, ao_dim), 1)
    cv_dup[...] = dot_t(one_hot(row == col), dup_t).astype(BF16)

    lane = iota((HALF, LANES), 1)
    lane_v = iota((virt, LANES), 1)
    lane_s = iota((SUB, LANES), 1)

    def quarter_step(index):
        slot = lax.rem(index, SLOTS)
        load(index).wait()
        for u in range(CHUNK):
            t_buf[u * 2 * HALF : (u + 1) * 2 * HALF, :] = dot(co_eo[...], a_buf[slot, u]).astype(BF16)

        @pl.when(index + SLOTS < rows * chunks)
        def _():
            load(index + SLOTS).start()

    def half_step(ch):
        for group in range(CHUNK // GROUP):
            h = dot(t_buf[group * GROUP * 2 * HALF : (group + 1) * GROUP * 2 * HALF, :], cv_dup[...])
            for u in range(GROUP):
                even = h[u * 2 * HALF : u * 2 * HALF + HALF]
                odd = h[u * 2 * HALF + HALF : (u + 1) * 2 * HALF]
                h_buf[pl.ds(ch * CHUNK + group * GROUP + u, HALF, stride=stride), :] = jnp.where(
                    lane < virt, even, odd
                )

    def row_step(p, carry):
        def chunk_step(ch, carry):
            half_step(ch - 1)
            quarter_step(p * chunks + ch)
            return carry

        quarter_step(p * chunks)
        lax.fori_loop(1, chunks, chunk_step, 0)
        half_step(chunks - 1)

        for first in range(0, pairs, 2):
            many = min(2, pairs - first)
            half_ints = jnp.concatenate(
                [h_buf[(first + w) * stride : (first + w) * stride + ao_dim, :].astype(BF16) for w in range(many)],
                axis=1,
            )
            g_buf[:, first * LANES : (first + many) * LANES] = dot(cv_t[...], half_ints)
        for d in range(n):
            start, offset = divmod(block * d, LANES)
            piece = g_buf[:, start * LANES : (start + 1) * LANES]
            if offset:
                piece = pltpu.roll(piece, LANES - offset, 1)
                if offset + block > LANES:
                    more = pltpu.roll(g_buf[:, (start + 1) * LANES : (start + 2) * LANES], LANES - offset, 1)
                    piece = jnp.where(lane_v < LANES - offset, piece, more)
            top = piece[kept:]
            packed = []
            for g in range(kept // SUB):
                part = piece[g * SUB : (g + 1) * SUB]
                if g < count:
                    part = jnp.where(lane_s < block, part, pltpu.roll(top, block - g * width, 1))
                packed.append(part)
            s_buf[p, d] = jnp.concatenate(packed, axis=0).astype(BF16)

        @pl.when(p == 0)
        def _():
            pl.semaphore_wait(barrier, n - 1)

        r_buf[p, me] = s_buf[p, me]

        for k in range(1, n):
            to = lax.rem(me + k, n)
            pltpu.make_async_remote_copy(
                src_ref=s_buf.at[p, to],
                dst_ref=r_buf.at[p, me],
                send_sem=s_sem.at[p],
                recv_sem=r_sem.at[p],
                device_id={"dev": to},
                device_id_type=MESH,
            ).start()

        return carry

    lax.fori_loop(0, rows, row_step, 0)

    m, k = occ * SUB, n * SUB
    row, col = iota((m, occ), 0), iota((m, occ), 1)
    wide = dot(one_hot(row // SUB == col), co_t[...]).astype(BF16)
    same = lax.rem(iota((m, k), 0), SUB) == lax.rem(iota((m, k), 1), SUB)
    for p in range(rows):
        row, col = iota((ao_dim, k), 0), iota((ao_dim, k), 1)
        spread = dot(wide, one_hot((col // SUB) * rows + p == row))
        kron[p] = jnp.where(same, spread, 0.0).astype(BF16)

    for p in range(rows):
        arrived = r_buf.at[p, pl.ds(0, n - 1)]
        pltpu.make_async_copy(arrived, arrived, r_sem.at[p]).wait()
        for first in range(0, kept // SUB, 2):
            many = min(2, kept // SUB - first)
            three_quarter = jnp.concatenate(
                [
                    r_buf[p, :, (first + w) * SUB : (first + w + 1) * SUB, :].reshape(n * SUB, LANES)
                    for w in range(many)
                ],
                axis=1,
            )
            v = dot(kron[p], three_quarter)
            for w in range(many):
                g = first + w
                part = v[:, w * LANES : (w + 1) * LANES]
                if p:
                    part = part + acc[g]
                if p < rows - 1 or g < count:
                    acc[g] = part
                if p == rows - 1:
                    out[:, g * SUB : (g + 1) * SUB, :] = part.reshape(occ, SUB, LANES)[:, :, :block]
    lane_m = iota((m, LANES), 1)
    top = pltpu.roll(acc[0], LANES - block, 1)
    for g in range(1, count):
        top = jnp.where(lane_m < g * width, top, pltpu.roll(acc[g], (g * width + LANES - block) % LANES, 1))
    out[:, kept:, :] = top.reshape(occ, SUB, LANES)[:, :, :block]

    for p in range(rows):
        sent = s_buf.at[p, pl.ds(0, n - 1)]
        pltpu.make_async_copy(sent, sent, s_sem.at[p]).wait()


def solution(mesh):
    n = mesh.shape["dev"]

    def local_part(ao_rows, occ_coef, virt_coef):
        rows, ao_dim = ao_rows.shape[0], ao_rows.shape[1]
        occ, virt = occ_coef.shape[1], virt_coef.shape[1]
        block = occ * virt // n
        kept = virt - SUB
        stride = ao_dim + 8
        hbm = pl.BlockSpec(memory_space=pltpu.HBM)
        return pl.pallas_call(
            functools.partial(kernel, n),
            out_shape=pltpu.VMEM((occ, virt, block), F32),
            in_specs=[hbm, hbm, hbm],
            out_specs=pl.BlockSpec(memory_space=pltpu.VMEM),
            scratch_shapes=[
                pltpu.VMEM((occ, ao_dim), BF16),
                pltpu.VMEM((virt, ao_dim), BF16),
                pltpu.VMEM((SLOTS, CHUNK, ao_dim, ao_dim), BF16),
                pltpu.VMEM((CHUNK * 2 * HALF, ao_dim), BF16),
                pltpu.VMEM((HALF * stride, LANES), F32),
                pltpu.VMEM((virt, occ * virt), F32),
                pltpu.VMEM((rows, n, kept, LANES), BF16),
                pltpu.VMEM((rows, n, kept, LANES), BF16),
                pltpu.VMEM((kept // SUB, occ * SUB, LANES), F32),
                pltpu.VMEM((rows, occ * SUB, n * SUB), BF16),
                pltpu.VMEM((2 * HALF, ao_dim), BF16),
                pltpu.VMEM((ao_dim, 2 * virt), BF16),
                pltpu.SemaphoreType.DMA((2,)),
                pltpu.SemaphoreType.DMA((SLOTS,)),
                pltpu.SemaphoreType.DMA((rows,)),
                pltpu.SemaphoreType.DMA((rows,)),
            ],
            compiler_params=pltpu.CompilerParams(
                collective_id=0, has_side_effects=True, vmem_limit_bytes=50 * 1024 * 1024
            ),
            name="transform",
        )(ao_rows, *[pltpu.with_memory_space_constraint(c, pltpu.HBM) for c in (occ_coef.T, virt_coef.T)])

    return jax.shard_map(
        local_part,
        mesh=mesh,
        in_specs=(P(("frag", "dev"), None, None, None), P("frag", None), P("frag", None)),
        out_specs=P("frag", None, "dev"),
        check_vma=False,
    )
```

```python
import functools

import jax
import jax.numpy as jnp
from jax import lax
from jax.experimental import pallas as pl
from jax.experimental.pallas import tpu as pltpu
from jax.sharding import PartitionSpec as P

MESH = pl.DeviceIdType.MESH
F32 = jnp.float32
BF16 = jnp.bfloat16
LANES = 128
SUB = 8
CHUNK = 16
GROUP = 4
SLOTS = 4
HALF = 32


def dot(a, b):
    return jnp.dot(a, b, preferred_element_type=F32)


def dot_t(a, b):
    return lax.dot_general(a, b, (((1,), (1,)), ((), ())), preferred_element_type=F32)


def iota(shape, dim):
    return lax.broadcasted_iota(jnp.int32, shape, dim)


def one_hot(condition):
    return jnp.where(condition, 1.0, 0.0).astype(BF16)


def fold_plan(block):
    count = -(-block // (LANES - block))
    assert block % count == 0
    return count, block // count


def kernel(
    n, ao, co_in, cv_in, out, co_t, cv_t, a_buf, t_buf, h_buf, g_buf, s_buf, r_buf, acc, kron, co_eo, cv_dup,
    c_sem, a_sem, s_sem, r_sem,
):
    rows, ao_dim = ao.shape[0], ao.shape[1]
    occ, virt = co_in.shape[0], cv_in.shape[0]
    block = out.shape[2]
    count, width = fold_plan(block)
    kept = virt - SUB
    pairs = occ // 2
    stride = h_buf.shape[0] // HALF
    chunks = ao_dim // CHUNK
    me = lax.axis_index("dev")
    barrier = pltpu.get_barrier_semaphore()

    coef = [pltpu.make_async_copy(co_in, co_t, c_sem.at[0]), pltpu.make_async_copy(cv_in, cv_t, c_sem.at[1])]
    for copy in coef:
        copy.start()

    def load(index):
        slot = lax.rem(index, SLOTS)
        return pltpu.make_async_copy(
            ao.at[index // chunks, pl.ds(lax.rem(index, chunks) * CHUNK, CHUNK)], a_buf.at[slot], a_sem.at[slot]
        )

    for index in range(SLOTS):
        load(jnp.int32(index)).start()

    @pl.loop(1, n)
    def _(k):
        pl.semaphore_signal(barrier, inc=1, device_id={"dev": lax.rem(me + k, n)}, device_id_type=MESH)

    for copy in coef:
        copy.wait()
    row, col = iota((2 * HALF, occ), 0), iota((2 * HALF, occ), 1)
    want = jnp.where(row < HALF, 2 * row, 2 * (row - HALF) + 1)
    co_eo[...] = dot(one_hot(want == col), co_t[...]).astype(BF16)
    row, col = iota((2 * virt, virt), 0), iota((2 * virt, virt), 1)
    dup_t = dot(one_hot(lax.rem(row, virt) == col), cv_t[...]).astype(BF16)
    row, col = iota((ao_dim, ao_dim), 0), iota((ao_dim, ao_dim), 1)
    cv_dup[...] = dot_t(one_hot(row == col), dup_t).astype(BF16)

    lane = iota((HALF, LANES), 1)
    lane_v = iota((virt, LANES), 1)
    lane_s = iota((SUB, LANES), 1)

    def quarter_step(index):
        slot = lax.rem(index, SLOTS)
        load(index).wait()
        for u in range(CHUNK):
            t_buf[u * 2 * HALF : (u + 1) * 2 * HALF, :] = dot(co_eo[...], a_buf[slot, u]).astype(BF16)

        @pl.when(index + SLOTS < rows * chunks)
        def _():
            load(index + SLOTS).start()

    def half_step(ch):
        for group in range(CHUNK // GROUP):
            h = dot(t_buf[group * GROUP * 2 * HALF : (group + 1) * GROUP * 2 * HALF, :], cv_dup[...])
            for u in range(GROUP):
                even = h[u * 2 * HALF : u * 2 * HALF + HALF]
                odd = h[u * 2 * HALF + HALF : (u + 1) * 2 * HALF]
                h_buf[pl.ds(ch * CHUNK + group * GROUP + u, HALF, stride=stride), :] = jnp.where(
                    lane < virt, even, odd
                )

    def row_step(p, carry):
        def chunk_step(ch, carry):
            half_step(ch - 1)
            quarter_step(p * chunks + ch)
            return carry

        quarter_step(p * chunks)
        lax.fori_loop(1, chunks, chunk_step, 0)
        half_step(chunks - 1)

        for first in range(0, pairs, 2):
            many = min(2, pairs - first)
            half_ints = jnp.concatenate(
                [h_buf[(first + w) * stride : (first + w) * stride + ao_dim, :].astype(BF16) for w in range(many)],
                axis=1,
            )
            g_buf[:, first * LANES : (first + many) * LANES] = dot(cv_t[...], half_ints)
        for d in range(n):
            start, offset = divmod(block * d, LANES)
            piece = g_buf[:, start * LANES : (start + 1) * LANES]
            if offset:
                piece = pltpu.roll(piece, LANES - offset, 1)
                if offset + block > LANES:
                    more = pltpu.roll(g_buf[:, (start + 1) * LANES : (start + 2) * LANES], LANES - offset, 1)
                    piece = jnp.where(lane_v < LANES - offset, piece, more)
            top = piece[kept:]
            packed = []
            for g in range(kept // SUB):
                part = piece[g * SUB : (g + 1) * SUB]
                if g < count:
                    part = jnp.where(lane_s < block, part, pltpu.roll(top, block - g * width, 1))
                packed.append(part)
            s_buf[p, d] = jnp.concatenate(packed, axis=0).astype(BF16)

        @pl.when(p == 0)
        def _():
            pl.semaphore_wait(barrier, n - 1)

        r_buf[p, me] = s_buf[p, me]

        for k in range(1, n):
            to = lax.rem(me + k, n)
            pltpu.make_async_remote_copy(
                src_ref=s_buf.at[p, to],
                dst_ref=r_buf.at[p, me],
                send_sem=s_sem.at[p],
                recv_sem=r_sem.at[p],
                device_id={"dev": to},
                device_id_type=MESH,
            ).start()

        return carry

    lax.fori_loop(0, rows, row_step, 0)

    m, k = occ * SUB, n * SUB
    row, col = iota((m, occ), 0), iota((m, occ), 1)
    wide = dot(one_hot(row // SUB == col), co_t[...]).astype(BF16)
    same = lax.rem(iota((m, k), 0), SUB) == lax.rem(iota((m, k), 1), SUB)
    for p in range(rows):
        row, col = iota((ao_dim, k), 0), iota((ao_dim, k), 1)
        spread = dot(wide, one_hot((col // SUB) * rows + p == row))
        kron[p] = jnp.where(same, spread, 0.0).astype(BF16)

    for p in range(rows):
        arrived = r_buf.at[p, pl.ds(0, n - 1)]
        pltpu.make_async_copy(arrived, arrived, r_sem.at[p]).wait()
        for first in range(0, kept // SUB, 2):
            many = min(2, kept // SUB - first)
            three_quarter = jnp.concatenate(
                [
                    r_buf[p, :, (first + w) * SUB : (first + w + 1) * SUB, :].reshape(n * SUB, LANES)
                    for w in range(many)
                ],
                axis=1,
            )
            v = dot(kron[p], three_quarter)
            for w in range(many):
                g = first + w
                part = v[:, w * LANES : (w + 1) * LANES]
                if p:
                    part = part + acc[g]
                if p < rows - 1 or g < count:
                    acc[g] = part
                if p == rows - 1:
                    out[:, g * SUB : (g + 1) * SUB, :] = part.reshape(occ, SUB, LANES)[:, :, :block]
    lane_m = iota((m, LANES), 1)
    top = pltpu.roll(acc[0], LANES - block, 1)
    for g in range(1, count):
        top = jnp.where(lane_m < g * width, top, pltpu.roll(acc[g], (g * width + LANES - block) % LANES, 1))
    out[:, kept:, :] = top.reshape(occ, SUB, LANES)[:, :, :block]

    for p in range(rows):
        sent = s_buf.at[p, pl.ds(0, n - 1)]
        pltpu.make_async_copy(sent, sent, s_sem.at[p]).wait()


def solution(mesh):
    n = mesh.shape["dev"]

    def local_part(ao_rows, occ_coef, virt_coef):
        rows, ao_dim = ao_rows.shape[0], ao_rows.shape[1]
        occ, virt = occ_coef.shape[1], virt_coef.shape[1]
        block = occ * virt // n
        kept = virt - SUB
        stride = ao_dim + 8
        hbm = pl.BlockSpec(memory_space=pltpu.HBM)
        return pl.pallas_call(
            functools.partial(kernel, n),
            out_shape=pltpu.VMEM((occ, virt, block), F32),
            in_specs=[hbm, hbm, hbm],
            out_specs=pl.BlockSpec(memory_space=pltpu.VMEM),
            scratch_shapes=[
                pltpu.VMEM((occ, ao_dim), BF16),
                pltpu.VMEM((virt, ao_dim), BF16),
                pltpu.VMEM((SLOTS, CHUNK, ao_dim, ao_dim), BF16),
                pltpu.VMEM((CHUNK * 2 * HALF, ao_dim), BF16),
                pltpu.VMEM((HALF * stride, LANES), F32),
                pltpu.VMEM((virt, occ * virt), F32),
                pltpu.VMEM((rows, n, kept, LANES), BF16),
                pltpu.VMEM((rows, n, kept, LANES), BF16),
                pltpu.VMEM((kept // SUB, occ * SUB, LANES), F32),
                pltpu.VMEM((rows, occ * SUB, n * SUB), BF16),
                pltpu.VMEM((2 * HALF, ao_dim), BF16),
                pltpu.VMEM((ao_dim, 2 * virt), BF16),
                pltpu.SemaphoreType.DMA((2,)),
                pltpu.SemaphoreType.DMA((SLOTS,)),
                pltpu.SemaphoreType.DMA((rows,)),
                pltpu.SemaphoreType.DMA((rows,)),
            ],
            compiler_params=pltpu.CompilerParams(
                collective_id=0, has_side_effects=True, vmem_limit_bytes=50 * 1024 * 1024
            ),
            name="transform",
        )(ao_rows, *[pltpu.with_memory_space_constraint(c, pltpu.HBM) for c in (occ_coef.T, virt_coef.T)])

    return jax.shard_map(
        local_part,
        mesh=mesh,
        in_specs=(P(("frag", "dev"), None, None, None), P("frag", None), P("frag", None)),
        out_specs=P("frag", None, "dev"),
        check_vma=False,
    )
```

```python
import functools

import jax
import jax.numpy as jnp
from jax import lax
from jax.experimental import pallas as pl
from jax.experimental.pallas import tpu as pltpu
from jax.sharding import PartitionSpec as P

MESH = pl.DeviceIdType.MESH
F32 = jnp.float32
BF16 = jnp.bfloat16
LANES = 128
SUB = 8
CHUNK = 32
GROUP = 4
SLOTS = 3
HALF = 32


def dot(a, b):
    return jnp.dot(a, b, preferred_element_type=F32)


def dot_t(a, b):
    return lax.dot_general(a, b, (((1,), (1,)), ((), ())), preferred_element_type=F32)


def iota(shape, dim):
    return lax.broadcasted_iota(jnp.int32, shape, dim)


def one_hot(condition):
    return jnp.where(condition, 1.0, 0.0).astype(BF16)


def fold_plan(block):
    count = -(-block // (LANES - block))
    assert block % count == 0
    return count, block // count


def kernel(
    n, ao, co_in, cv_in, out, co_t, cv_t, a_buf, t_buf, h_buf, g_buf, s_buf, r_buf, acc, kron, co_eo, cv_dup,
    c_sem, a_sem, s_sem, r_sem,
):
    rows, ao_dim = ao.shape[0], ao.shape[1]
    occ, virt = co_in.shape[0], cv_in.shape[0]
    block = out.shape[2]
    count, width = fold_plan(block)
    kept = virt - SUB
    pairs = occ // 2
    stride = h_buf.shape[0] // HALF
    chunks = ao_dim // CHUNK
    me = lax.axis_index("dev")
    barrier = pltpu.get_barrier_semaphore()

    coef = [pltpu.make_async_copy(co_in, co_t, c_sem.at[0]), pltpu.make_async_copy(cv_in, cv_t, c_sem.at[1])]
    for copy in coef:
        copy.start()

    def load(index):
        slot = lax.rem(index, SLOTS)
        return pltpu.make_async_copy(
            ao.at[index // chunks, pl.ds(lax.rem(index, chunks) * CHUNK, CHUNK)], a_buf.at[slot], a_sem.at[slot]
        )

    for index in range(SLOTS):
        load(jnp.int32(index)).start()

    @pl.loop(1, n)
    def _(k):
        pl.semaphore_signal(barrier, inc=1, device_id={"dev": lax.rem(me + k, n)}, device_id_type=MESH)

    for copy in coef:
        copy.wait()
    row, col = iota((2 * HALF, occ), 0), iota((2 * HALF, occ), 1)
    want = jnp.where(row < HALF, 2 * row, 2 * (row - HALF) + 1)
    co_eo[...] = dot(one_hot(want == col), co_t[...]).astype(BF16)
    row, col = iota((2 * virt, virt), 0), iota((2 * virt, virt), 1)
    dup_t = dot(one_hot(lax.rem(row, virt) == col), cv_t[...]).astype(BF16)
    row, col = iota((ao_dim, ao_dim), 0), iota((ao_dim, ao_dim), 1)
    cv_dup[...] = dot_t(one_hot(row == col), dup_t).astype(BF16)

    lane = iota((HALF, LANES), 1)
    lane_v = iota((virt, LANES), 1)
    lane_s = iota((SUB, LANES), 1)

    def quarter_step(index):
        slot = lax.rem(index, SLOTS)
        load(index).wait()
        for u in range(CHUNK):
            t_buf[u * 2 * HALF : (u + 1) * 2 * HALF, :] = dot(co_eo[...], a_buf[slot, u]).astype(BF16)

        @pl.when(index + SLOTS < rows * chunks)
        def _():
            load(index + SLOTS).start()

    def half_step(ch):
        for group in range(CHUNK // GROUP):
            h = dot(t_buf[group * GROUP * 2 * HALF : (group + 1) * GROUP * 2 * HALF, :], cv_dup[...])
            for u in range(GROUP):
                even = h[u * 2 * HALF : u * 2 * HALF + HALF]
                odd = h[u * 2 * HALF + HALF : (u + 1) * 2 * HALF]
                h_buf[pl.ds(ch * CHUNK + group * GROUP + u, HALF, stride=stride), :] = jnp.where(
                    lane < virt, even, odd
                )

    def row_step(p, carry):
        def chunk_step(ch, carry):
            half_step(ch - 1)
            quarter_step(p * chunks + ch)
            return carry

        quarter_step(p * chunks)
        lax.fori_loop(1, chunks, chunk_step, 0)
        half_step(chunks - 1)

        for first in range(0, pairs, 2):
            many = min(2, pairs - first)
            half_ints = jnp.concatenate(
                [h_buf[(first + w) * stride : (first + w) * stride + ao_dim, :].astype(BF16) for w in range(many)],
                axis=1,
            )
            g_buf[:, first * LANES : (first + many) * LANES] = dot(cv_t[...], half_ints)
        for d in range(n):
            start, offset = divmod(block * d, LANES)
            piece = g_buf[:, start * LANES : (start + 1) * LANES]
            if offset:
                piece = pltpu.roll(piece, LANES - offset, 1)
                if offset + block > LANES:
                    more = pltpu.roll(g_buf[:, (start + 1) * LANES : (start + 2) * LANES], LANES - offset, 1)
                    piece = jnp.where(lane_v < LANES - offset, piece, more)
            top = piece[kept:]
            packed = []
            for g in range(kept // SUB):
                part = piece[g * SUB : (g + 1) * SUB]
                if g < count:
                    part = jnp.where(lane_s < block, part, pltpu.roll(top, block - g * width, 1))
                packed.append(part)
            s_buf[p, d] = jnp.concatenate(packed, axis=0).astype(BF16)

        @pl.when(p == 0)
        def _():
            pl.semaphore_wait(barrier, n - 1)

        r_buf[p, me] = s_buf[p, me]

        for k in range(1, n):
            to = lax.rem(me + k, n)
            pltpu.make_async_remote_copy(
                src_ref=s_buf.at[p, to],
                dst_ref=r_buf.at[p, me],
                send_sem=s_sem.at[p],
                recv_sem=r_sem.at[p],
                device_id={"dev": to},
                device_id_type=MESH,
            ).start()

        return carry

    lax.fori_loop(0, rows, row_step, 0)

    m, k = occ * SUB, n * SUB
    row, col = iota((m, occ), 0), iota((m, occ), 1)
    wide = dot(one_hot(row // SUB == col), co_t[...]).astype(BF16)
    same = lax.rem(iota((m, k), 0), SUB) == lax.rem(iota((m, k), 1), SUB)
    for p in range(rows):
        row, col = iota((ao_dim, k), 0), iota((ao_dim, k), 1)
        spread = dot(wide, one_hot((col // SUB) * rows + p == row))
        kron[p] = jnp.where(same, spread, 0.0).astype(BF16)

    for p in range(rows):
        arrived = r_buf.at[p, pl.ds(0, n - 1)]
        pltpu.make_async_copy(arrived, arrived, r_sem.at[p]).wait()
        for first in range(0, kept // SUB, 2):
            many = min(2, kept // SUB - first)
            three_quarter = jnp.concatenate(
                [
                    r_buf[p, :, (first + w) * SUB : (first + w + 1) * SUB, :].reshape(n * SUB, LANES)
                    for w in range(many)
                ],
                axis=1,
            )
            v = dot(kron[p], three_quarter)
            for w in range(many):
                g = first + w
                part = v[:, w * LANES : (w + 1) * LANES]
                if p:
                    part = part + acc[g]
                if p < rows - 1 or g < count:
                    acc[g] = part
                if p == rows - 1:
                    out[:, g * SUB : (g + 1) * SUB, :] = part.reshape(occ, SUB, LANES)[:, :, :block]
    lane_m = iota((m, LANES), 1)
    top = pltpu.roll(acc[0], LANES - block, 1)
    for g in range(1, count):
        top = jnp.where(lane_m < g * width, top, pltpu.roll(acc[g], (g * width + LANES - block) % LANES, 1))
    out[:, kept:, :] = top.reshape(occ, SUB, LANES)[:, :, :block]

    for p in range(rows):
        sent = s_buf.at[p, pl.ds(0, n - 1)]
        pltpu.make_async_copy(sent, sent, s_sem.at[p]).wait()


def solution(mesh):
    n = mesh.shape["dev"]

    def local_part(ao_rows, occ_coef, virt_coef):
        rows, ao_dim = ao_rows.shape[0], ao_rows.shape[1]
        occ, virt = occ_coef.shape[1], virt_coef.shape[1]
        block = occ * virt // n
        kept = virt - SUB
        stride = ao_dim + 4
        hbm = pl.BlockSpec(memory_space=pltpu.HBM)
        return pl.pallas_call(
            functools.partial(kernel, n),
            out_shape=pltpu.VMEM((occ, virt, block), F32),
            in_specs=[hbm, hbm, hbm],
            out_specs=pl.BlockSpec(memory_space=pltpu.VMEM),
            scratch_shapes=[
                pltpu.VMEM((occ, ao_dim), BF16),
                pltpu.VMEM((virt, ao_dim), BF16),
                pltpu.VMEM((SLOTS, CHUNK, ao_dim, ao_dim), BF16),
                pltpu.VMEM((CHUNK * 2 * HALF, ao_dim), BF16),
                pltpu.VMEM((HALF * stride, LANES), F32),
                pltpu.VMEM((virt, occ * virt), F32),
                pltpu.VMEM((rows, n, kept, LANES), BF16),
                pltpu.VMEM((rows, n, kept, LANES), BF16),
                pltpu.VMEM((kept // SUB, occ * SUB, LANES), F32),
                pltpu.VMEM((rows, occ * SUB, n * SUB), BF16),
                pltpu.VMEM((2 * HALF, ao_dim), BF16),
                pltpu.VMEM((ao_dim, 2 * virt), BF16),
                pltpu.SemaphoreType.DMA((2,)),
                pltpu.SemaphoreType.DMA((SLOTS,)),
                pltpu.SemaphoreType.DMA((rows,)),
                pltpu.SemaphoreType.DMA((rows,)),
            ],
            compiler_params=pltpu.CompilerParams(
                collective_id=0, has_side_effects=True, vmem_limit_bytes=50 * 1024 * 1024
            ),
            name="transform",
        )(ao_rows, *[pltpu.with_memory_space_constraint(c, pltpu.HBM) for c in (occ_coef.T, virt_coef.T)])

    return jax.shard_map(
        local_part,
        mesh=mesh,
        in_specs=(P(("frag", "dev"), None, None, None), P("frag", None), P("frag", None)),
        out_specs=P("frag", None, "dev"),
        check_vma=False,
    )
```
